16 devices in a mesh: tp: 2 (over z), dp: 8 (over y, x, core).
Axes of the slice: x: 2, y: 2, z: 2, core: 2. Of those that a mesh axis runs over, the one named last changes fastest.
Arguments:
- h_teacher: bfloat16 [32768, 4096], P('dp')
- h_student: bfloat16 [32768, 4096], P('dp')
- w_teacher: bfloat16 [4096, 4096], P(None, 'tp')
- w_student: bfloat16 [4096, 4096], P(None, 'tp')
Outputs:
- output 1: float32 [], replicated
- output 2: float32 [32768, 4096], P('dp')
- output 3: float32 [4096, 4096], P(None, 'tp')
All inputs are finite; a program needn't handle non-finite values.
Results may differ from the reference program's by a relative error of at most 0.001.
Values sent between devices are 32-bit elements.
A program may use at most 1 GiB of HBM per device.

```python
import jax
import jax.numpy as jnp
from jax import lax

TOKENS = 32768
VOCAB = 4096
D_TEACHER = 4096
D_STUDENT = 4096
ROW_BLOCK = 256


def setup_inputs(seed: int = 0) -> dict:
    root_key = jax.random.key(seed)
    key_ht, key_hs, key_wt, key_ws = jax.random.split(root_key, 4)
    h_teacher = jax.random.normal(key_ht, (TOKENS, D_TEACHER), jnp.float32)
    h_student = jax.random.normal(key_hs, (TOKENS, D_STUDENT), jnp.float32)
    w_teacher = jax.random.normal(key_wt, (D_TEACHER, VOCAB), jnp.float32) * (2.0 * D_TEACHER ** -0.5)
    w_student = jax.random.normal(key_ws, (D_STUDENT, VOCAB), jnp.float32) * (1.5 * D_STUDENT ** -0.5)
    return {
        "h_teacher": h_teacher.astype(jnp.bfloat16),
        "h_student": h_student.astype(jnp.bfloat16),
        "w_teacher": w_teacher.astype(jnp.bfloat16),
        "w_student": w_student.astype(jnp.bfloat16),
    }


def log_probs(logits):
    row_max = jnp.max(logits, axis=1, keepdims=True)
    shifted = logits - row_max
    exp_vals = jnp.exp(shifted)
    row_sum = jnp.sum(exp_vals, axis=1, keepdims=True)
    return exp_vals / row_sum, shifted - jnp.log(row_sum)


def reference(h_teacher, h_student, w_teacher, w_student):
    num_blocks = TOKENS // ROW_BLOCK
    ht_blocks = h_teacher.reshape(num_blocks, ROW_BLOCK, D_TEACHER)
    hs_blocks = h_student.reshape(num_blocks, ROW_BLOCK, D_STUDENT)

    def scan_step(dw_acc, block_pair):
        ht_block, hs_block = block_pair
        prob_t, logp_t = log_probs(jnp.dot(ht_block, w_teacher, preferred_element_type=jnp.float32))
        prob_s, logp_s = log_probs(jnp.dot(hs_block, w_student, preferred_element_type=jnp.float32))
        kl_rows = jnp.sum(prob_t * (logp_t - logp_s), axis=1)
        dz_student = ((prob_s - prob_t) / TOKENS).astype(jnp.bfloat16)
        dh_block = jnp.dot(dz_student, w_student.T, preferred_element_type=jnp.float32)
        dw_acc = dw_acc + jnp.dot(hs_block.T, dz_student, preferred_element_type=jnp.float32)
        return dw_acc, (kl_rows, dh_block)

    dw_start = jnp.zeros((D_STUDENT, VOCAB), jnp.float32)
    dw_student, (kl_rows, dh_blocks) = lax.scan(scan_step, dw_start, (ht_blocks, hs_blocks))
    kl_loss = jnp.sum(kl_rows) / TOKENS
    return kl_loss, dh_blocks.reshape(TOKENS, D_STUDENT), dw_student
```

```python
import functools

import jax
import jax.numpy as jnp
from jax import lax
from jax.experimental import pallas as pl
from jax.experimental.pallas import tpu as pltpu
from jax.sharding import PartitionSpec as P


F32 = jnp.float32
BF16 = jnp.bfloat16
BM = 256
FM = 512
CN = 512
LANES = 128
SHARED_BLOCKS = 5
W_PIECES = 2
VMEM_LIMIT = 60 * 1024 * 1024


def _dot(a, b):
    return jnp.dot(a, b, preferred_element_type=F32)


def _fwd_kernel(slot, h_ref, w_ref, prev_ref, *rest):
    z_ref, st_ref = rest[-2:]
    rows = h_ref.shape[0]
    run_max = jnp.full((rows, LANES), -jnp.inf, F32)
    run_sum = jnp.zeros((rows, LANES), F32)
    for c in range(w_ref.shape[1] // CN):
        z = _dot(h_ref[...], w_ref[:, c * CN:(c + 1) * CN])
        z_ref[:, c * CN:(c + 1) * CN] = z
        parts = [z[:, k * LANES:(k + 1) * LANES] for k in range(CN // LANES)]
        new_max = run_max
        for part in parts:
            new_max = jnp.maximum(new_max, part)
        run_sum = run_sum * jnp.exp(run_max - new_max)
        for part in parts:
            run_sum = run_sum + jnp.exp(part - new_max)
        run_max = new_max
    row_max = jnp.max(run_max, axis=1, keepdims=True)
    row_sum = jnp.sum(run_sum * jnp.exp(run_max - row_max), axis=1, keepdims=True)
    lane = lax.broadcasted_iota(jnp.int32, (rows, LANES), 1)
    packed = jnp.where(lane == slot, row_max, jnp.where(lane == slot + 1, row_sum, 0.0))
    st_ref[...] = prev_ref[...] + packed.T[:8, :]


def _row_stats(st_ref):
    a, b = st_ref[0], st_ref[1]
    rows = []
    for k in (0, 2):
        m_a, s_a, m_b, s_b = a[k:k + 1], a[k + 1:k + 2], b[k:k + 1], b[k + 1:k + 2]
        m = jnp.maximum(m_a, m_b)
        s = s_a * jnp.exp(m_a - m) + s_b * jnp.exp(m_b - m)
        rows += [m, 1.0 / s, jnp.log(s)]
    flat = jnp.concatenate(rows + [jnp.zeros((LANES - len(rows), BM), F32)], axis=0)
    cols = flat.T
    return [cols[:, k:k + 1] for k in range(6)]


def _dz_kernel(tok_total, zt_ref, zs_ref, st_ref, *rest):
    dz_ref, share_ref, kl_ref = rest[-3:]
    m_t, r_t, l_t, m_s, r_s, l_s = _row_stats(st_ref)
    kl = jnp.zeros((8, LANES), F32)
    for c in range(zt_ref.shape[1] // CN):
        cs = slice(c * CN, (c + 1) * CN)
        shift_t = zt_ref[:, cs] - m_t
        shift_s = zs_ref[:, cs] - m_s
        p_t = jnp.exp(shift_t) * r_t
        p_s = jnp.exp(shift_s) * r_s
        dz_ref[:, cs] = ((p_s - p_t) * (1.0 / tok_total)).astype(BF16)
        term = p_t * ((shift_t - l_t) - (shift_s - l_s))
        term = term[:, :256] + term[:, 256:]
        term = term[:, :LANES] + term[:, LANES:]
        kl = kl + jnp.sum(term.reshape(BM // 8, 8, LANES), axis=0)

    @pl.when(pl.program_id(0) == 0)
    def _():
        kl_ref[...] = jnp.zeros_like(kl_ref)

    @pl.when(pl.program_id(0) < SHARED_BLOCKS)
    def _():
        share_ref[...] = dz_ref[...].astype(F32)

    kl_ref[...] += kl


def _narrow_kernel(*refs):
    per_piece = pl.num_programs(0) // W_PIECES
    out_ref = refs[-1]
    for j in range(W_PIECES):
        @pl.when(pl.program_id(0) // per_piece == j)
        def _(j=j):
            out_ref[...] = refs[j][...].astype(BF16)


def _far_kernel(tok_total, ht_ref, hs_ref, wt_ref, ws_ref, st_ref, got_ref, kl_in_ref, _, dz_ref, kl_ref):
    i = pl.program_id(0)
    kl_ref[...] = kl_in_ref[...]

    @pl.when(i < SHARED_BLOCKS)
    def _():
        dz_ref[...] = got_ref[...].astype(BF16)

    @pl.when(i >= SHARED_BLOCKS)
    def _():
        m_t, r_t, _, m_s, r_s, _ = _row_stats(st_ref)
        for c in range(dz_ref.shape[1] // CN):
            cs = slice(c * CN, (c + 1) * CN)
            p_t = jnp.exp(_dot(ht_ref[...], wt_ref[:, cs]) - m_t) * r_t
            p_s = jnp.exp(_dot(hs_ref[...], ws_ref[:, cs]) - m_s) * r_s
            dz_ref[:, cs] = ((p_s - p_t) * (1.0 / tok_total)).astype(BF16)


def _resident(shape):
    return pl.BlockSpec(shape, lambda i: (0, 0), pipeline_mode=pl.Buffered(1))


def _untouched():
    return pl.BlockSpec(memory_space=pl.ANY)


def _params():
    return pltpu.CompilerParams(dimension_semantics=("arbitrary",), vmem_limit_bytes=VMEM_LIMIT)


def solution(mesh):
    tp_size, dp_size = mesh.shape["tp"], mesh.shape["dp"]
    swap = [(k, (k + 1) % tp_size) for k in range(tp_size)]

    def local_step(h_teacher, h_student, w_teacher, w_student):
        tokens, depth = h_teacher.shape
        vocab = w_teacher.shape[1]
        tok_total = tokens * dp_size
        blocks = tokens // BM
        shared = SHARED_BLOCKS * BM
        unit = 2 * tokens * depth * vocab

        dp_index = lax.axis_index("dp")
        piece = depth // W_PIECES
        part = piece // dp_size

        def far_slices(w):
            out = []
            for j in range(W_PIECES):
                mine = lax.dynamic_slice_in_dim(w, j * piece + dp_index * part, part, axis=0)
                out.append(lax.ppermute(mine.astype(F32), "tp", swap))
            return out

        def far_gather(slices):
            out = []
            for theirs in slices:
                out.append(lax.all_gather(theirs, "dp", axis=0, tiled=True))
            return out

        def narrow(wide):
            per_piece = piece // BM
            return pl.pallas_call(
                _narrow_kernel,
                grid=(depth // BM,),
                in_specs=[pl.BlockSpec((BM, vocab),
                                       lambda i, j=j: (jnp.clip(i - j * per_piece, 0, per_piece - 1), 0))
                          for j in range(W_PIECES)],
                out_specs=pl.BlockSpec((BM, vocab), lambda i: (i, 0)),
                out_shape=jax.ShapeDtypeStruct((depth, vocab), BF16),
                compiler_params=_params(),
                cost_estimate=pl.CostEstimate(flops=unit // 4, bytes_accessed=48 << 20, transcendentals=0),
                name="narrow",
            )(*wide)

        def forward(slot, h, w, prev, first, count, into=None):
            base = first // FM
            held = [] if into is None else list(into)
            rows = lambda i: (i + base, 0)
            lanes = lambda i: (0, i + base)
            return pl.pallas_call(
                functools.partial(_fwd_kernel, slot),
                grid=(count // FM,),
                in_specs=[pl.BlockSpec((FM, depth), rows),
                          _resident((depth, vocab)),
                          pl.BlockSpec((8, FM), lanes)] + [_untouched()] * len(held),
                out_specs=[pl.BlockSpec((FM, vocab), rows), pl.BlockSpec((8, FM), lanes)],
                out_shape=[jax.ShapeDtypeStruct((tokens, vocab), F32),
                           jax.ShapeDtypeStruct((8, tokens), F32)],
                input_output_aliases={3: 0, 4: 1} if held else {},
                compiler_params=_params(),
                cost_estimate=pl.CostEstimate(flops=unit * count // tokens,
                                              bytes_accessed=(16 << 20) + (64 << 20) * count // tokens,
                                              transcendentals=0),
                name="fwd",
            )(h, w, prev, *held)

        slices_t = far_slices(w_teacher)
        slices_s = far_slices(w_student)
        wide_t = far_gather(slices_t)
        wide_s = far_gather(slices_s)

        none = jnp.zeros((8, tokens), F32)
        half = tokens // 2
        start = forward(0, h_teacher, w_teacher, none, 0, half)
        z_t, stats_t = forward(0, h_teacher, w_teacher, none, half, half, start)
        z_s, stats = forward(2, h_student, w_student, stats_t, 0, tokens)

        both = lax.all_gather(stats, "tp")

        dz_own, share, kl_part = pl.pallas_call(
            functools.partial(_dz_kernel, tok_total),
            grid=(blocks,),
            in_specs=[pl.BlockSpec((BM, vocab), lambda i: (i, 0)),
                      pl.BlockSpec((BM, vocab), lambda i: (i, 0)),
                      pl.BlockSpec((tp_size, 8, BM), lambda i: (0, 0, i))],
            out_specs=[pl.BlockSpec((BM, vocab), lambda i: (i, 0)),
                       pl.BlockSpec((BM, vocab), lambda i: (jnp.minimum(i, SHARED_BLOCKS - 1), 0)),
                       pl.BlockSpec((8, LANES), lambda i: (0, 0))],
            out_shape=[jax.ShapeDtypeStruct((tokens, vocab), BF16),
                       jax.ShapeDtypeStruct((shared, vocab), F32),
                       jax.ShapeDtypeStruct((8, LANES), F32)],
            compiler_params=_params(),
            cost_estimate=pl.CostEstimate(flops=unit // 3, bytes_accessed=90 << 20, transcendentals=0),
            name="dz_own",
        )(z_t, z_s, both)

        got = lax.ppermute(share, "tp", swap)

        dw_part = lax.dot_general(h_student, dz_own, (((0,), (0,)), ((), ())),
                                  preferred_element_type=F32)
        dw_student = lax.psum(dw_part, "dp")

        dh_own = lax.dot_general(dz_own, w_student, (((1,), (1,)), ((), ())),
                                 preferred_element_type=F32)

        far_t = narrow(wide_t)
        far_s = narrow(wide_s)

        dz_far, kl_part = pl.pallas_call(
            functools.partial(_far_kernel, tok_total),
            grid=(blocks,),
            in_specs=[pl.BlockSpec((BM, depth), lambda i: (jnp.maximum(i, SHARED_BLOCKS), 0)),
                      pl.BlockSpec((BM, depth), lambda i: (jnp.maximum(i, SHARED_BLOCKS), 0))]
            + [_resident((depth, vocab))] * 2
            + [pl.BlockSpec((tp_size, 8, BM), lambda i: (0, 0, i)),
               pl.BlockSpec((BM, vocab), lambda i: (jnp.minimum(i, SHARED_BLOCKS - 1), 0)),
               pl.BlockSpec((8, LANES), lambda i: (0, 0)), _untouched()],
            out_specs=[pl.BlockSpec((BM, vocab), lambda i: (i, 0)),
                       pl.BlockSpec((8, LANES), lambda i: (0, 0))],
            out_shape=[jax.ShapeDtypeStruct((tokens, vocab), BF16),
                       jax.ShapeDtypeStruct((8, LANES), F32)],
            compiler_params=_params(),
            cost_estimate=pl.CostEstimate(flops=2 * unit * (blocks - SHARED_BLOCKS) // blocks,
                                          bytes_accessed=112 << 20, transcendentals=0),
            name="dz_far",
        )(h_teacher, h_student, far_t, far_s, both, got, kl_part, dh_own)

        kl_loss = lax.psum(jnp.sum(kl_part), ("tp", "dp")) / tok_total

        dh_student = dh_own + lax.dot_general(dz_far, far_s, (((1,), (1,)), ((), ())),
                                              preferred_element_type=F32)
        return kl_loss, dh_student, dw_student

    return jax.shard_map(
        local_step, mesh=mesh,
        in_specs=(P("dp", None), P("dp", None), P(None, "tp"), P(None, "tp")),
        out_specs=(P(), P("dp", None), P(None, "tp")),
        check_vma=False)
```
